256 devices in a mesh: pb: 8 (over x, core), ga: 32 (over y, z).
Axes of the slice: x: 4, y: 4, z: 8, core: 2. Of those that a mesh axis runs over, the one named last changes fastest.
Arguments:
- queries: bfloat16 [16384, 512], P(('pb', 'ga')), may hold values from -4 to 4
- gallery: bfloat16 [49152, 512], P('ga'), may hold values from -1 to 1
- positives: int32 [16384, 4], P('pb'), may hold values from 0 to 49151, as said below
- cutoffs: int32 [4], replicated, may hold values from 1 to 1537
Outputs:
- query_grad: float32 [16384, 512], P(('pb', 'ga'))
- gallery_grad: float32 [49152, 512], P(('ga', 'pb'))
The draws below stay inside these ranges and needn't reach their ends.
Inputs may be any that keep to these rules, and one draw needn't show every extreme that they name: `positives`: indices of a query may repeat.
All inputs are finite; a program needn't handle non-finite values.
Results may differ from the reference program's by a relative error of at most 0.0043.
Values may be sent and summed in bfloat16 or wider, within the bound.
No kernel may reach another device: no remote copies, remote signals or barrier semaphores. Data moves between devices by JAX's collectives and lax.ppermute only.
A program may use at most 64 MiB of HBM per device.

```python
import jax
import jax.numpy as jnp
from jax import lax

D = 512
NPOS = 4
NCUT = 4
Q = 16384
G = 49152


def common_draw(key):
    base = jax.random.fold_in(key, 911)
    key_gallery, key_pos, key_strength, key_noise = jax.random.split(base, 4)
    positives = jax.random.randint(key_pos, (Q, NPOS), 0, G, dtype=jnp.int32)
    gallery = jnp.clip(jax.random.normal(key_gallery, (G, D), jnp.float32), -4.0, 4.0) * D ** (-0.5)
    gallery = gallery.astype(jnp.bfloat16).astype(jnp.float32)
    strength = jnp.exp(jax.random.uniform(key_strength, (Q, 1), jnp.float32, jnp.log(0.2), jnp.log(0.7)))
    summed = jnp.sum(gallery[positives], axis=1)
    noise = jax.random.normal(key_noise, (Q, D), jnp.float32) * D ** (-0.5)
    queries = jnp.clip(strength * summed + noise, -4.0, 4.0)
    return (gallery, positives, queries)


def draw_gallery(key, part):
    return common_draw(key)[0].astype(jnp.bfloat16)


def draw_positives(key, part):
    return common_draw(key)[1]


def draw_queries(key, part):
    return common_draw(key)[2].astype(jnp.bfloat16)


def touch_ends(array, key, least, high):
    longest = array.shape.index(max(array.shape))
    spots = []
    for shift in (0, 1):
        where = [jax.random.randint(jax.random.fold_in(key, axis), (), 0, length) for axis, length in enumerate(array.shape)]
        where[longest] = (where[longest] + shift) % array.shape[longest]
        spots.append(tuple(where))
    return array.at[spots[0]].set(least).at[spots[1]].set(high)


def setup_inputs(seed: int = 0) -> dict:
    seeds = jax.random.split(jax.random.key(seed), 5)
    queries = draw_queries(jax.random.fold_in(seeds[4], 71), 0)
    gallery = draw_gallery(jax.random.fold_in(seeds[4], 71), 0)
    positives = draw_positives(jax.random.fold_in(seeds[4], 71), 0)
    cutoffs = touch_ends(jax.random.randint(seeds[3], (NCUT,), 1, G // 32 + 2), jax.random.fold_in(seeds[3], 1), 1, (G // 32 + 2) - 1).astype(jnp.int32)
    return {"queries": queries, "gallery": gallery, "positives": positives, "cutoffs": cutoffs}


TEMP = 0.05
SHARP = 4.0


def reference(queries, gallery, positives, cutoffs):
    block_rows = min(512, Q)
    blocks = Q // block_rows
    cut_values = cutoffs.astype(jnp.float32)

    def handle(gallery_acc, pieces):
        query_block, pos_block = pieces
        scores = jnp.dot(query_block, gallery.T, preferred_element_type=jnp.float32)
        anchor = jnp.take_along_axis(scores, pos_block, axis=1)
        counted = []
        slopes = []
        for member in range(NPOS):
            squash = jax.nn.sigmoid((scores - anchor[:, member:member + 1]) / TEMP)
            counted.append(0.5 + jnp.sum(squash, axis=1))
            slopes.append(jnp.sum(squash * (1.0 - squash), axis=1) / TEMP)
        rank_total = jnp.stack(counted, axis=1)
        slope_total = jnp.stack(slopes, axis=1)
        recall = jax.nn.sigmoid(SHARP * (cut_values - rank_total[:, :, None]) / cut_values)
        weight_rank = jnp.sum(recall * (1.0 - recall) * SHARP / cut_values, axis=-1) / (NPOS * NCUT)
        weight = jnp.zeros(scores.shape, jnp.float32)
        for member in range(NPOS):
            squash = jax.nn.sigmoid((scores - anchor[:, member:member + 1]) / TEMP)
            weight = weight + weight_rank[:, member:member + 1] * squash * (1.0 - squash) / TEMP
        row_index = jnp.arange(block_rows, dtype=jnp.int32)[:, None]
        weight = weight.at[row_index, pos_block].add(-weight_rank * slope_total)
        dscore = weight.astype(jnp.bfloat16)
        query_part = jnp.dot(dscore, gallery, preferred_element_type=jnp.float32)
        gallery_acc = gallery_acc + jnp.dot(dscore.T, query_block, preferred_element_type=jnp.float32)
        return gallery_acc, query_part

    start_acc = jnp.zeros((G, D), jnp.float32)
    gallery_grad, query_parts = lax.scan(
        handle, start_acc,
        (queries.reshape(blocks, block_rows, D), positives.reshape(blocks, block_rows, NPOS)))
    return query_parts.reshape(Q, D), gallery_grad
```

```python
import functools

import jax
import jax.numpy as jnp
from jax import lax
from jax.experimental import pallas as pl
from jax.experimental.pallas import tpu as pltpu
from jax.sharding import Mesh, PartitionSpec as P

TEMP = 0.05
SHARP = 4.0
HALF_INV = 0.5 / TEMP
TILE = 256
CHUNK = 64
F32 = jnp.float32
BF16 = jnp.bfloat16


def shift(value, axis, step):
    peers = lax.axis_size(axis)
    return lax.ppermute(value, axis, [(i, (i + step) % peers) for i in range(peers)])


def score_body(*refs):
    gallery_ref, query_ref, index_ref, score_ref, anchor_ref = refs[-5:]
    rows, lanes = score_ref.shape
    members = index_ref.shape[0]
    score_ref[...] = (
        lax.dot_general(gallery_ref[...], query_ref[...], (((1,), (1,)), ((), ())), preferred_element_type=F32)
        * HALF_INV
    )
    iota = lax.broadcasted_iota(jnp.int32, (CHUNK, lanes), 0)

    def step(i, found):
        base = i * CHUNK
        part = score_ref[pl.ds(pl.multiple_of(base, CHUNK), CHUNK), :]
        new = []
        for m in range(members):
            hit = iota == (index_ref[m : m + 1, :] - base)
            picked = jnp.where(hit, part, 0.0)
            new.append(found[m] + jnp.sum(picked.reshape(CHUNK // 8, 8, lanes), axis=0))
        return tuple(new)

    zero = jnp.zeros((8, lanes), F32)
    found = lax.fori_loop(0, rows // CHUNK, step, (zero,) * members)
    for m in range(members):
        anchor_ref[m : m + 1, :] = jnp.sum(found[m], axis=0, keepdims=True)


def score_block(gallery, queries, index, scores, slot, slots):
    rows, width = gallery.shape
    count = queries.shape[0]
    members = index.shape[0]
    steps = count // TILE
    first = scores is None
    in_specs = [
        pl.BlockSpec((rows, width), lambda i: (0, 0)),
        pl.BlockSpec((TILE, width), lambda i: (i, 0)),
        pl.BlockSpec((members, TILE), lambda i: (0, i)),
    ]
    args = [gallery, queries, index]
    aliases = {}
    if not first:
        in_specs = [pl.BlockSpec(memory_space=pl.ANY), *in_specs]
        args = [scores, *args]
        aliases = {0: 0}
    return pl.pallas_call(
        score_body,
        grid=(steps,),
        in_specs=in_specs,
        out_specs=[
            pl.BlockSpec((rows, TILE), lambda i: (0, slot * steps + i)),
            pl.BlockSpec((members, TILE), lambda i: (0, i)),
        ],
        out_shape=[
            jax.ShapeDtypeStruct((rows, slots * count), F32),
            jax.ShapeDtypeStruct((members, count), F32),
        ],
        input_output_aliases=aliases,
        name=f"scores{slot}",
    )(*args)


def rank_body(score_ref, anchor_ref, stat_ref):
    rows, lanes = score_ref.shape
    members = anchor_ref.shape[0]
    groups = CHUNK // 8
    for lane in range(0, lanes, 128):
        anchors = [anchor_ref[m : m + 1, lane : lane + 128] for m in range(members)]

        def step(i, sums):
            part = score_ref[pl.ds(pl.multiple_of(i * CHUNK, CHUNK), CHUNK), lane : lane + 128]
            new = []
            for m in range(members):
                t = jnp.tanh(part - anchors[m])
                new.append(sums[2 * m] + (jnp.sum(t.reshape(groups, 8, 128), axis=0) + float(groups)))
                new.append(sums[2 * m + 1] + (float(groups) - jnp.sum((t * t).reshape(groups, 8, 128), axis=0)))
            return tuple(new)

        zero = jnp.zeros((8, 128), F32)
        sums = lax.fori_loop(0, rows // CHUNK, step, (zero,) * (2 * members), unroll=2)
        for m in range(members):
            stat_ref[m : m + 1, lane : lane + 128] = 0.5 * jnp.sum(sums[2 * m], axis=0, keepdims=True)
            stat_ref[members + m : members + m + 1, lane : lane + 128] = 0.25 * jnp.sum(
                sums[2 * m + 1], axis=0, keepdims=True
            )


def rank_sums(scores, anchors):
    rows, count = scores.shape
    members = anchors.shape[0]
    return pl.pallas_call(
        rank_body,
        grid=(count // TILE,),
        in_specs=[
            pl.BlockSpec((rows, TILE), lambda i: (0, i)),
            pl.BlockSpec((members, TILE), lambda i: (0, i)),
        ],
        out_specs=pl.BlockSpec((2 * members, TILE), lambda i: (0, i)),
        out_shape=jax.ShapeDtypeStruct((2 * members, count), F32),
        name="rank_sums",
    )(scores, anchors)


def weight_body(*refs):
    cut_ref, score_ref, anchor_ref, index_ref, stat_ref, gallery_ref, dscore_ref, query_ref, coef_ref = refs[-9:]
    rows, lanes = score_ref.shape
    members = anchor_ref.shape[0]
    cuts = cut_ref.shape[0]
    rank = 0.5 + stat_ref[0:members, :]
    slope = stat_ref[members : 2 * members, :] / TEMP
    weight = jnp.zeros((members, lanes), F32)
    for c in range(cuts):
        cut = cut_ref[c].astype(F32)
        decay = jnp.exp(-jnp.abs(SHARP * (cut - rank) / cut))
        weight = weight + decay / ((1.0 + decay) * (1.0 + decay)) * (SHARP / cut)
    weight = weight / float(members * cuts)
    scaled = weight * (0.25 / TEMP)
    coef_ref[0:members, :] = scaled
    coef_ref[members : 2 * members, :] = weight * slope
    total = jnp.sum(scaled, axis=0, keepdims=True)
    iota = lax.broadcasted_iota(jnp.int32, (CHUNK, 128), 0)
    for lane in range(0, lanes, 128):
        span = slice(lane, lane + 128)
        base_total = total[:, span]

        def step(i, carry):
            base = pl.multiple_of(i * CHUNK, CHUNK)
            part = score_ref[pl.ds(base, CHUNK), span]
            acc = jnp.broadcast_to(base_total, (CHUNK, 128))
            for m in range(members):
                t = jnp.tanh(part - anchor_ref[m : m + 1, span])
                hit = iota == (index_ref[m : m + 1, span] - base)
                acc = acc - jnp.where(
                    hit, coef_ref[members + m : members + m + 1, span], coef_ref[m : m + 1, span] * (t * t)
                )
            dscore_ref[pl.ds(base, CHUNK), span] = acc.astype(BF16)
            return carry

        lax.fori_loop(0, rows // CHUNK, step, 0)
    query_ref[...] = lax.dot_general(
        dscore_ref[...], gallery_ref[...], (((0,), (0,)), ((), ())), preferred_element_type=F32
    ).astype(query_ref.dtype)


def weight_block(cutoffs, scores, anchors, index, stats, gallery, dscore, slot, slots, dtype):
    rows, width = gallery.shape
    members = anchors.shape[0]
    count = scores.shape[1] // slots
    steps = count // TILE
    here = lambda i: (0, slot * steps + i)
    in_specs = [
        pl.BlockSpec(memory_space=pltpu.SMEM),
        pl.BlockSpec((rows, TILE), here),
        pl.BlockSpec((members, TILE), here),
        pl.BlockSpec((members, TILE), here),
        pl.BlockSpec((2 * members, TILE), here),
        pl.BlockSpec((rows, width), lambda i: (0, 0)),
    ]
    args = [cutoffs, scores, anchors, index, stats, gallery]
    aliases = {}
    if dscore is not None:
        in_specs = [pl.BlockSpec(memory_space=pl.ANY), *in_specs]
        args = [dscore, *args]
        aliases = {0: 0}
    return pl.pallas_call(
        weight_body,
        grid=(steps,),
        in_specs=in_specs,
        out_specs=[pl.BlockSpec((rows, TILE), here), pl.BlockSpec((TILE, width), lambda i: (i, 0))],
        out_shape=[
            jax.ShapeDtypeStruct((rows, slots * count), BF16),
            jax.ShapeDtypeStruct((count, width), dtype),
        ],
        scratch_shapes=[pltpu.VMEM((2 * members, TILE), F32)],
        input_output_aliases=aliases,
        name=f"weights{slot}",
    )(*args)


def gallery_body(dscore_ref, *refs):
    out_ref = refs[-1]
    at = 0
    acc = None
    for query_ref in refs[:-1]:
        size = query_ref.shape[0]
        term = jnp.dot(dscore_ref[:, at : at + size], query_ref[...], preferred_element_type=F32)
        acc = term if acc is None else acc + term
        at += size
    out_ref[...] = acc.astype(out_ref.dtype)


def gallery_terms(dscore, parts):
    rows, count = dscore.shape
    width = parts[0].shape[1]
    tile = rows // 8
    return pl.pallas_call(
        gallery_body,
        grid=(rows // tile,),
        in_specs=[
            pl.BlockSpec((tile, count), lambda i: (i, 0)),
            *[pl.BlockSpec(p.shape, lambda i: (0, 0)) for p in parts],
        ],
        out_specs=pl.BlockSpec((tile, width), lambda i: (i, 0)),
        out_shape=jax.ShapeDtypeStruct((rows, width), F32),
        name="gallery_terms",
    )(dscore, *parts)


def summed_over_gallery(value):
    size = value.shape[1] // lax.axis_size("y")
    parts = [jnp.roll(shift(value, "y", k), -k * size, axis=1) for k in range(1, lax.axis_size("y"))]
    for part in parts:
        value = value + part
    step = 1
    while step < lax.axis_size("z"):
        value = value + lax.ppermute(value, "z", [(i, i ^ step) for i in range(lax.axis_size("z"))])
        step *= 2
    return value


def shards(queries, gallery, positives, cutoffs):
    ny = lax.axis_size("y")
    nz = lax.axis_size("z")
    nx = lax.axis_size("x")
    yy = lax.axis_index("y")
    gallery_rows, width = gallery.shape
    first_row = (yy * nz + lax.axis_index("z")) * gallery_rows
    local = positives.T - first_row
    size = local.shape[1] // ny
    local = lax.dynamic_slice_in_dim(jnp.concatenate([local, local], axis=1), yy * size, ny * size, 1)

    copies = jnp.broadcast_to(queries[None], (nz, *queries.shape))
    own = lax.all_to_all(copies, "z", 0, 0, tiled=True).reshape(size, width)
    half = size // 2
    after = shift(own, "y", -1)
    before = shift(own, "y", 1)
    far_a = shift(after[:half], "y", -1)
    far_b = shift(before[half:], "y", 1)
    far = jnp.concatenate([far_a, far_b], axis=0)
    blocks = [own, after, far, before]

    scores = None
    anchors = [None] * ny
    for slot in (0, 1, 3, 2):
        index = local[:, slot * size : (slot + 1) * size]
        scores, anchors[slot] = score_block(gallery, blocks[slot], index, scores, slot, ny)
    anchors = summed_over_gallery(jnp.concatenate(anchors, axis=1))
    stats = summed_over_gallery(rank_sums(scores, anchors))

    weights = functools.partial(weight_block, cutoffs, scores, anchors, local, stats, gallery)
    dscore, part_far = weights(None, 2, ny, BF16)
    got_a = shift(part_far[:half], "y", 1)
    got_b = shift(part_far[half:], "y", -1)
    dscore, part_after = weights(dscore, 1, ny, F32)
    dscore, part_before = weights(dscore, 3, ny, F32)
    up = jnp.concatenate([part_after[:half] + got_a.astype(F32), part_after[half:]], axis=0).astype(BF16)
    down = jnp.concatenate([part_before[:half], part_before[half:] + got_b.astype(F32)], axis=0).astype(BF16)
    got_up = shift(up, "y", 1)
    got_down = shift(down, "y", -1)
    dscore, part_own = weights(dscore, 0, ny, F32)
    gallery_part = gallery_terms(dscore, blocks)

    out_rows = gallery_rows // (2 * nx)
    split = gallery_part.reshape(nx, 2, out_rows, width)
    core = lax.axis_index("c")
    mine = lax.dynamic_index_in_dim(split, core, 1, False)
    other = lax.dynamic_index_in_dim(split, 1 - core, 1, False).astype(BF16)
    pair = mine + lax.ppermute(other, "c", [(0, 1), (1, 0)]).astype(F32)
    xx = lax.axis_index("x")
    gallery_grad = lax.dynamic_index_in_dim(pair, xx, 0, False)
    sent = [
        shift(lax.dynamic_index_in_dim(pair, (xx + k) % nx, 0, False).astype(BF16), "x", k) for k in range(1, nx)
    ]
    for part in sent:
        gallery_grad = gallery_grad + part.astype(F32)

    query_part = (part_own + got_up.astype(F32) + got_down.astype(F32)).astype(BF16)
    landed = lax.all_to_all(query_part.reshape(nz, size // nz, width), "z", 0, 0, tiled=True)
    query_grad = jnp.sum(landed.astype(F32), axis=0)
    return (query_grad, gallery_grad)


def solution(mesh):
    fine = Mesh(mesh.devices.reshape(4, 2, 4, 8), ("x", "c", "y", "z"))
    placed = (P(("x", "c", "y", "z"), None), P(("y", "z"), None), P(("x", "c"), None), P())
    return jax.shard_map(
        shards,
        mesh=fine,
        in_specs=placed,
        out_specs=(P(("x", "c", "y", "z"), None), P(("y", "z", "x", "c"), None)),
        check_vma=False,
    )
```

```python
import functools

import jax
import jax.numpy as jnp
from jax import lax
from jax.experimental import pallas as pl
from jax.experimental.pallas import tpu as pltpu
from jax.sharding import Mesh, PartitionSpec as P

TEMP = 0.05
SHARP = 4.0
HALF_INV = 0.5 / TEMP
TILE = 256
CHUNK = 64
F32 = jnp.float32
BF16 = jnp.bfloat16


def priced(micros):
    return pl.CostEstimate(flops=int(micros * 5e8), transcendentals=0, bytes_accessed=int(micros * 1e6))


def shift(value, axis, step):
    peers = lax.axis_size(axis)
    return lax.ppermute(value, axis, [(i, (i + step) % peers) for i in range(peers)])


def score_body(*refs):
    gallery_ref, query_ref, index_ref, score_ref, anchor_ref = refs[-5:]
    rows, lanes = score_ref.shape
    members = index_ref.shape[0]
    score_ref[...] = (
        lax.dot_general(gallery_ref[...], query_ref[...], (((1,), (1,)), ((), ())), preferred_element_type=F32)
        * HALF_INV
    )
    iota = lax.broadcasted_iota(jnp.int32, (CHUNK, lanes), 0)

    def step(i, found):
        base = i * CHUNK
        part = score_ref[pl.ds(pl.multiple_of(base, CHUNK), CHUNK), :]
        new = []
        for m in range(members):
            wanted = index_ref[m : m + 1, :] - base
            best = found[m]
            for row in range(0, CHUNK, 8):
                best = jnp.where(iota[row : row + 8] == wanted, part[row : row + 8], best)
            new.append(best)
        return tuple(new)

    zero = jnp.zeros((8, lanes), F32)
    found = lax.fori_loop(0, rows // CHUNK, step, (zero,) * members)
    for m in range(members):
        anchor_ref[m : m + 1, :] = jnp.sum(found[m], axis=0, keepdims=True)


def score_block(gallery, queries, index, scores, slot, slots):
    rows, width = gallery.shape
    count = queries.shape[0]
    members = index.shape[0]
    steps = count // TILE
    first = scores is None
    in_specs = [
        pl.BlockSpec((rows, width), lambda i: (0, 0)),
        pl.BlockSpec((TILE, width), lambda i: (i, 0)),
        pl.BlockSpec((members, TILE), lambda i: (0, i)),
    ]
    args = [gallery, queries, index]
    aliases = {}
    if not first:
        in_specs = [pl.BlockSpec(memory_space=pl.ANY), *in_specs]
        args = [scores, *args]
        aliases = {0: 0}
    return pl.pallas_call(
        score_body,
        grid=(steps,),
        in_specs=in_specs,
        out_specs=[
            pl.BlockSpec((rows, TILE), lambda i: (0, slot * steps + i)),
            pl.BlockSpec((members, TILE), lambda i: (0, i)),
        ],
        out_shape=[
            jax.ShapeDtypeStruct((rows, slots * count), F32),
            jax.ShapeDtypeStruct((members, count), F32),
        ],
        input_output_aliases=aliases,
        cost_estimate=priced(5),
    )(*args)


def rank_body(score_ref, anchor_ref, stat_ref):
    rows, lanes = score_ref.shape
    members = anchor_ref.shape[0]
    groups = CHUNK // 8
    for lane in range(0, lanes, 128):
        anchors = [anchor_ref[m : m + 1, lane : lane + 128] for m in range(members)]

        def step(i, sums):
            part = score_ref[pl.ds(pl.multiple_of(i * CHUNK, CHUNK), CHUNK), lane : lane + 128]
            new = []
            for m in range(members):
                t = jnp.tanh(part - anchors[m])
                new.append(sums[2 * m] + (jnp.sum(t.reshape(groups, 8, 128), axis=0) + float(groups)))
                new.append(sums[2 * m + 1] + (float(groups) - jnp.sum((t * t).reshape(groups, 8, 128), axis=0)))
            return tuple(new)

        zero = jnp.zeros((8, 128), F32)
        sums = lax.fori_loop(0, rows // CHUNK, step, (zero,) * (2 * members), unroll=4)
        for m in range(members):
            stat_ref[m : m + 1, lane : lane + 128] = 0.5 * jnp.sum(sums[2 * m], axis=0, keepdims=True)
            stat_ref[members + m : members + m + 1, lane : lane + 128] = 0.25 * jnp.sum(
                sums[2 * m + 1], axis=0, keepdims=True
            )


def rank_sums(scores, anchors):
    rows, count = scores.shape
    members = anchors.shape[0]
    return pl.pallas_call(
        rank_body,
        grid=(count // TILE,),
        in_specs=[
            pl.BlockSpec((rows, TILE), lambda i: (0, i)),
            pl.BlockSpec((members, TILE), lambda i: (0, i)),
        ],
        out_specs=pl.BlockSpec((2 * members, TILE), lambda i: (0, i)),
        out_shape=jax.ShapeDtypeStruct((2 * members, count), F32),
        cost_estimate=priced(12),
        name="rank_sums",
    )(scores, anchors)


def weight_body(*refs):
    cut_ref, score_ref, anchor_ref, index_ref, stat_ref, gallery_ref, dscore_ref, query_ref, coef_ref = refs[-9:]
    rows, lanes = score_ref.shape
    members = anchor_ref.shape[0]
    cuts = cut_ref.shape[0]
    rank = 0.5 + stat_ref[0:members, :]
    slope = stat_ref[members : 2 * members, :] / TEMP
    weight = jnp.zeros((members, lanes), F32)
    for c in range(cuts):
        cut = cut_ref[c].astype(F32)
        decay = jnp.exp(-jnp.abs(SHARP * (cut - rank) / cut))
        weight = weight + decay / ((1.0 + decay) * (1.0 + decay)) * (SHARP / cut)
    weight = weight / float(members * cuts)
    scaled = weight * (0.25 / TEMP)
    coef_ref[0:members, :] = scaled
    coef_ref[members : 2 * members, :] = weight * slope
    total = jnp.sum(scaled, axis=0, keepdims=True)
    iota = lax.broadcasted_iota(jnp.int32, (CHUNK, 128), 0)
    for lane in range(0, lanes, 128):
        span = slice(lane, lane + 128)
        base_total = total[:, span]

        def step(i, carry):
            base = pl.multiple_of(i * CHUNK, CHUNK)
            part = score_ref[pl.ds(base, CHUNK), span]
            acc = jnp.broadcast_to(base_total, (CHUNK, 128))
            for m in range(members):
                t = jnp.tanh(part - anchor_ref[m : m + 1, span])
                hit = iota == (index_ref[m : m + 1, span] - base)
                acc = acc - jnp.where(
                    hit, coef_ref[members + m : members + m + 1, span], coef_ref[m : m + 1, span] * (t * t)
                )
            dscore_ref[pl.ds(base, CHUNK), span] = acc.astype(BF16)
            return carry

        lax.fori_loop(0, rows // CHUNK, step, 0, unroll=2)
    turned = jnp.dot(gallery_ref[...], dscore_ref[...], preferred_element_type=F32)
    query_ref[...] = turned.T.astype(query_ref.dtype)


def weight_blocks(cutoffs, scores, anchors, index, stats, turned, dscore, which, slots, dtype):
    width, rows = turned.shape
    members = anchors.shape[0]
    count = scores.shape[1] // slots
    steps = count // TILE
    stride = which[-1] - which[0] if len(which) > 1 else 0
    here = lambda i: (0, (which[0] + stride * (i // steps)) * steps + i % steps)
    in_specs = [
        pl.BlockSpec(memory_space=pltpu.SMEM),
        pl.BlockSpec((rows, TILE), here),
        pl.BlockSpec((members, TILE), here),
        pl.BlockSpec((members, TILE), here),
        pl.BlockSpec((2 * members, TILE), here),
        pl.BlockSpec((width, rows), lambda i: (0, 0)),
    ]
    args = [cutoffs, scores, anchors, index, stats, turned]
    aliases = {}
    if dscore is not None:
        in_specs = [pl.BlockSpec(memory_space=pl.ANY), *in_specs]
        args = [dscore, *args]
        aliases = {0: 0}
    return pl.pallas_call(
        weight_body,
        grid=(steps * len(which),),
        in_specs=in_specs,
        out_specs=[pl.BlockSpec((rows, TILE), here), pl.BlockSpec((TILE, width), lambda i: (i, 0))],
        out_shape=[
            jax.ShapeDtypeStruct((rows, slots * count), BF16),
            jax.ShapeDtypeStruct((len(which) * count, width), dtype),
        ],
        scratch_shapes=[pltpu.VMEM((2 * members, TILE), F32)],
        input_output_aliases=aliases,
        cost_estimate=priced(6 * len(which)),
    )(*args)


def gallery_body(dscore_ref, *refs):
    out_ref = refs[-1]
    at = 0
    acc = None
    for query_ref in refs[:-1]:
        size = query_ref.shape[0]
        term = jnp.dot(dscore_ref[:, at : at + size], query_ref[...], preferred_element_type=F32)
        acc = term if acc is None else acc + term
        at += size
    out_ref[...] = acc.astype(out_ref.dtype)


def gallery_terms(dscore, parts):
    rows, count = dscore.shape
    width = parts[0].shape[1]
    tile = rows // 3
    return pl.pallas_call(
        gallery_body,
        grid=(rows // tile,),
        in_specs=[
            pl.BlockSpec((tile, count), lambda i: (i, 0)),
            *[pl.BlockSpec(p.shape, lambda i: (0, 0)) for p in parts],
        ],
        out_specs=pl.BlockSpec((tile, width), lambda i: (i, 0)),
        out_shape=jax.ShapeDtypeStruct((rows, width), F32),
        cost_estimate=priced(6),
        name="gallery_terms",
    )(dscore, *parts)


def summed_over_gallery(value):
    size = value.shape[1] // lax.axis_size("y")
    parts = [jnp.roll(shift(value, "y", k), -k * size, axis=1) for k in range(1, lax.axis_size("y"))]
    for part in parts:
        value = value + part
    lower = shift(value, "z", 1)
    upper = shift(value, "z", -1)
    two = value + lower
    three = two + upper
    return three + shift(three, "z", 3) + shift(two, "z", -3)


def shard_terms(queries, gallery, positives, cutoffs):
    ny = lax.axis_size("y")
    nz = lax.axis_size("z")
    nx = lax.axis_size("x")
    yy = lax.axis_index("y")
    gallery_rows, width = gallery.shape
    first_row = (yy * nz + lax.axis_index("z")) * gallery_rows
    local = positives.T - first_row
    size = local.shape[1] // ny
    local = lax.dynamic_slice_in_dim(jnp.concatenate([local, local], axis=1), yy * size, ny * size, 1)

    copies = jnp.broadcast_to(queries[None], (nz, *queries.shape))
    own = lax.all_to_all(copies, "z", 0, 0, tiled=True).reshape(size, width)
    half = size // 2
    after = shift(own, "y", -1)
    before = shift(own, "y", 1)
    far_a = shift(after[:half], "y", -1)
    far_b = shift(before[half:], "y", 1)
    far = jnp.concatenate([far_a, far_b], axis=0)
    blocks = [own, after, far, before]

    scores = None
    anchors = [None] * ny
    for slot in (0, 1, 3, 2):
        index = local[:, slot * size : (slot + 1) * size]
        scores, anchors[slot] = score_block(gallery, blocks[slot], index, scores, slot, ny)
    anchors = summed_over_gallery(jnp.concatenate(anchors, axis=1))
    stats = summed_over_gallery(rank_sums(scores, anchors))

    weights = functools.partial(weight_blocks, cutoffs, scores, anchors, local, stats, gallery.T)
    dscore, part_far = weights(None, (2,), ny, BF16)
    got_a = shift(part_far[:half], "y", 1)
    got_b = shift(part_far[half:], "y", -1)
    dscore, part_next = weights(dscore, (1, 3), ny, F32)
    part_after, part_before = part_next[:size], part_next[size:]
    up = jnp.concatenate([part_after[:half] + got_a.astype(F32), part_after[half:]], axis=0).astype(BF16)
    down = jnp.concatenate([part_before[:half], part_before[half:] + got_b.astype(F32)], axis=0).astype(BF16)
    dscore, up, down = lax.optimization_barrier((dscore, up, down))
    got_up = shift(up, "y", 1)
    got_down = shift(down, "y", -1)
    dscore, part_own = weights(dscore, (0,), ny, F32)
    gallery_part = gallery_terms(dscore, blocks)

    out_rows = gallery_rows // (2 * nx)
    split = gallery_part.reshape(nx, 2, out_rows, width)
    core = lax.axis_index("c")
    mine = lax.dynamic_index_in_dim(split, core, 1, False)
    other = lax.dynamic_index_in_dim(split, 1 - core, 1, False).astype(BF16)
    pair = mine + lax.ppermute(other, "c", [(0, 1), (1, 0)]).astype(F32)
    xx = lax.axis_index("x")
    gallery_grad = lax.dynamic_index_in_dim(pair, xx, 0, False)
    sent = [
        shift(lax.dynamic_index_in_dim(pair, (xx + k) % nx, 0, False).astype(BF16), "x", k) for k in range(1, nx)
    ]
    for part in sent:
        gallery_grad = gallery_grad + part.astype(F32)

    query_part = (part_own + got_up.astype(F32) + got_down.astype(F32)).astype(BF16)
    landed = lax.all_to_all(query_part.reshape(nz, size // nz, width), "z", 0, 0, tiled=True)
    query_grad = jnp.sum(landed.astype(F32), axis=0)
    return (query_grad, gallery_grad)


def solution(mesh):
    fine = Mesh(mesh.devices.reshape(4, 2, 4, 8), ("x", "c", "y", "z"))
    placed = (P(("x", "c", "y", "z"), None), P(("y", "z"), None), P(("x", "c"), None), P())
    return jax.shard_map(
        shard_terms,
        mesh=fine,
        in_specs=placed,
        out_specs=(P(("x", "c", "y", "z"), None), P(("y", "z", "x", "c"), None)),
        check_vma=False,
    )
```

```python
import functools

import jax
import jax.numpy as jnp
from jax import lax
from jax.experimental import pallas as pl
from jax.experimental.pallas import tpu as pltpu
from jax.sharding import Mesh, PartitionSpec as P

TEMP = 0.05
SHARP = 4.0
HALF_INV = 0.5 / TEMP
TILE = 256
CHUNK = 64
F32 = jnp.float32
BF16 = jnp.bfloat16


def priced(micros):
    return pl.CostEstimate(flops=int(micros * 5e8), transcendentals=0, bytes_accessed=int(micros * 1e6))


def near(value):
    return pltpu.with_memory_space_constraint(value, pltpu.MemorySpace.VMEM)


def shift(value, axis, step):
    peers = lax.axis_size(axis)
    return lax.ppermute(value, axis, [(i, (i + step) % peers) for i in range(peers)])


def score_body(*refs):
    gallery_ref, query_ref, index_ref, score_ref, anchor_ref = refs[-5:]
    rows, lanes = score_ref.shape
    members = index_ref.shape[0]
    score_ref[...] = (
        lax.dot_general(gallery_ref[...], query_ref[...], (((1,), (1,)), ((), ())), preferred_element_type=F32)
        * HALF_INV
    )
    iota = lax.broadcasted_iota(jnp.int32, (CHUNK, lanes), 0)

    def step(i, found):
        base = i * CHUNK
        part = score_ref[pl.ds(pl.multiple_of(base, CHUNK), CHUNK), :]
        new = []
        for m in range(members):
            wanted = index_ref[m : m + 1, :] - base
            best = found[m]
            for row in range(0, CHUNK, 8):
                best = jnp.where(iota[row : row + 8] == wanted, part[row : row + 8], best)
            new.append(best)
        return tuple(new)

    zero = jnp.zeros((8, lanes), F32)
    found = lax.fori_loop(0, rows // CHUNK, step, (zero,) * members)
    for m in range(members):
        anchor_ref[m : m + 1, :] = jnp.sum(found[m], axis=0, keepdims=True)


def score_block(gallery, queries, index, scores, slot, slots):
    rows, width = gallery.shape
    count = queries.shape[0]
    members = index.shape[0]
    steps = count // TILE
    first = scores is None
    in_specs = [
        pl.BlockSpec((rows, width), lambda i: (0, 0)),
        pl.BlockSpec((TILE, width), lambda i: (i, 0)),
        pl.BlockSpec((members, TILE), lambda i: (0, i)),
    ]
    args = [gallery, queries, index]
    aliases = {}
    if not first:
        in_specs = [pl.BlockSpec(memory_space=pl.ANY), *in_specs]
        args = [scores, *args]
        aliases = {0: 0}
    return pl.pallas_call(
        score_body,
        grid=(steps,),
        in_specs=in_specs,
        out_specs=[
            pl.BlockSpec((rows, TILE), lambda i: (0, slot * steps + i)),
            pl.BlockSpec((members, TILE), lambda i: (0, i)),
        ],
        out_shape=[
            jax.ShapeDtypeStruct((rows, slots * count), F32),
            jax.ShapeDtypeStruct((members, count), F32),
        ],
        input_output_aliases=aliases,
        cost_estimate=priced(5),
        compiler_params=pltpu.CompilerParams(vmem_limit_bytes=12 * 2**20),
    )(*args)


def rank_body(score_ref, anchor_ref, stat_ref):
    rows, lanes = score_ref.shape
    members = anchor_ref.shape[0]
    groups = CHUNK // 8
    for lane in range(0, lanes, 128):
        anchors = [anchor_ref[m : m + 1, lane : lane + 128] for m in range(members)]

        def step(i, sums):
            part = score_ref[pl.ds(pl.multiple_of(i * CHUNK, CHUNK), CHUNK), lane : lane + 128]
            new = []
            for m in range(members):
                t = jnp.tanh(part - anchors[m])
                new.append(sums[2 * m] + (jnp.sum(t.reshape(groups, 8, 128), axis=0) + float(groups)))
                new.append(sums[2 * m + 1] + (float(groups) - jnp.sum((t * t).reshape(groups, 8, 128), axis=0)))
            return tuple(new)

        zero = jnp.zeros((8, 128), F32)
        sums = lax.fori_loop(0, rows // CHUNK, step, (zero,) * (2 * members), unroll=4)
        for m in range(members):
            stat_ref[m : m + 1, lane : lane + 128] = 0.5 * jnp.sum(sums[2 * m], axis=0, keepdims=True)
            stat_ref[members + m : members + m + 1, lane : lane + 128] = 0.25 * jnp.sum(
                sums[2 * m + 1], axis=0, keepdims=True
            )


def rank_sums(scores, anchors):
    rows, count = scores.shape
    members = anchors.shape[0]
    return pl.pallas_call(
        rank_body,
        grid=(count // TILE,),
        in_specs=[
            pl.BlockSpec((rows, TILE), lambda i: (0, i)),
            pl.BlockSpec((members, TILE), lambda i: (0, i)),
        ],
        out_specs=pl.BlockSpec((2 * members, TILE), lambda i: (0, i)),
        out_shape=jax.ShapeDtypeStruct((2 * members, count), F32),
        cost_estimate=priced(12),
        compiler_params=pltpu.CompilerParams(vmem_limit_bytes=8 * 2**20),
        name="rank_sums",
    )(scores, anchors)


def weight_body(*refs):
    cut_ref, score_ref, anchor_ref, index_ref, stat_ref, gallery_ref, dscore_ref, query_ref, coef_ref = refs[-9:]
    rows, lanes = score_ref.shape
    members = anchor_ref.shape[0]
    cuts = cut_ref.shape[0]
    rank = 0.5 + stat_ref[0:members, :]
    slope = stat_ref[members : 2 * members, :] / TEMP
    weight = jnp.zeros((members, lanes), F32)
    for c in range(cuts):
        cut = cut_ref[c].astype(F32)
        decay = jnp.exp(-jnp.abs(SHARP * (cut - rank) / cut))
        weight = weight + decay / ((1.0 + decay) * (1.0 + decay)) * (SHARP / cut)
    weight = weight / float(members * cuts)
    scaled = weight * (0.25 / TEMP)
    coef_ref[0:members, :] = scaled
    coef_ref[members : 2 * members, :] = weight * slope
    total = jnp.sum(scaled, axis=0, keepdims=True)
    iota = lax.broadcasted_iota(jnp.int32, (CHUNK, 128), 0)
    for lane in range(0, lanes, 128):
        span = slice(lane, lane + 128)
        base_total = total[:, span]

        def step(i, carry):
            base = pl.multiple_of(i * CHUNK, CHUNK)
            part = score_ref[pl.ds(base, CHUNK), span]
            acc = jnp.broadcast_to(base_total, (CHUNK, 128))
            for m in range(members):
                t = jnp.tanh(part - anchor_ref[m : m + 1, span])
                hit = iota == (index_ref[m : m + 1, span] - base)
                acc = acc - jnp.where(
                    hit, coef_ref[members + m : members + m + 1, span], coef_ref[m : m + 1, span] * (t * t)
                )
            dscore_ref[pl.ds(base, CHUNK), span] = acc.astype(BF16)
            return carry

        lax.fori_loop(0, rows // CHUNK, step, 0, unroll=2)
    turned = jnp.dot(gallery_ref[...], dscore_ref[...], preferred_element_type=F32)
    query_ref[...] = turned.T.astype(query_ref.dtype)


def weight_blocks(cutoffs, scores, anchors, index, stats, turned, dscore, which, slots, dtype):
    width, rows = turned.shape
    members = anchors.shape[0]
    count = scores.shape[1] // slots
    steps = count // TILE
    stride = which[-1] - which[0] if len(which) > 1 else 0
    here = lambda i: (0, (which[0] + stride * (i // steps)) * steps + i % steps)
    in_specs = [
        pl.BlockSpec(memory_space=pltpu.SMEM),
        pl.BlockSpec((rows, TILE), here),
        pl.BlockSpec((members, TILE), here),
        pl.BlockSpec((members, TILE), here),
        pl.BlockSpec((2 * members, TILE), here),
        pl.BlockSpec((width, rows), lambda i: (0, 0)),
    ]
    args = [cutoffs, scores, anchors, index, stats, turned]
    aliases = {}
    if dscore is not None:
        in_specs = [pl.BlockSpec(memory_space=pl.ANY), *in_specs]
        args = [dscore, *args]
        aliases = {0: 0}
    return pl.pallas_call(
        weight_body,
        grid=(steps * len(which),),
        in_specs=in_specs,
        out_specs=[pl.BlockSpec((rows, TILE), here), pl.BlockSpec((TILE, width), lambda i: (i, 0))],
        out_shape=[
            jax.ShapeDtypeStruct((rows, slots * count), BF16),
            jax.ShapeDtypeStruct((len(which) * count, width), dtype),
        ],
        scratch_shapes=[pltpu.VMEM((2 * members, TILE), F32)],
        input_output_aliases=aliases,
        cost_estimate=priced(6 * len(which)),
        compiler_params=pltpu.CompilerParams(vmem_limit_bytes=16 * 2**20),
    )(*args)


def gallery_body(dscore_ref, *refs):
    out_ref = refs[-1]
    at = 0
    acc = None
    for query_ref in refs[:-1]:
        size = query_ref.shape[0]
        term = jnp.dot(dscore_ref[:, at : at + size], query_ref[...], preferred_element_type=F32)
        acc = term if acc is None else acc + term
        at += size
    out_ref[...] = acc.astype(out_ref.dtype)


def gallery_terms(dscore, parts):
    rows, count = dscore.shape
    width = parts[0].shape[1]
    tile = rows // 3
    return pl.pallas_call(
        gallery_body,
        grid=(rows // tile,),
        in_specs=[
            pl.BlockSpec((tile, count), lambda i: (i, 0)),
            *[pl.BlockSpec(p.shape, lambda i: (0, 0)) for p in parts],
        ],
        out_specs=pl.BlockSpec((tile, width), lambda i: (i, 0)),
        out_shape=jax.ShapeDtypeStruct((rows, width), F32),
        cost_estimate=priced(6),
        compiler_params=pltpu.CompilerParams(vmem_limit_bytes=20 * 2**20),
        name="gallery_terms",
    )(dscore, *parts)


def summed_over_gallery(value):
    size = value.shape[1] // lax.axis_size("y")
    parts = [jnp.roll(shift(value, "y", k), -k * size, axis=1) for k in range(1, lax.axis_size("y"))]
    for part in parts:
        value = value + part
    lower = shift(value, "z", 1)
    upper = shift(value, "z", -1)
    two = value + lower
    three = two + upper
    return three + shift(three, "z", 3) + shift(two, "z", -3)


def shard_terms(queries, gallery, positives, cutoffs):
    ny = lax.axis_size("y")
    nz = lax.axis_size("z")
    nx = lax.axis_size("x")
    yy = lax.axis_index("y")
    gallery_rows, width = gallery.shape
    first_row = (yy * nz + lax.axis_index("z")) * gallery_rows
    local = positives.T - first_row
    size = local.shape[1] // ny
    local = lax.dynamic_slice_in_dim(jnp.concatenate([local, local], axis=1), yy * size, ny * size, 1)

    copies = jnp.broadcast_to(queries[None], (nz, *queries.shape))
    own = lax.all_to_all(copies, "z", 0, 0, tiled=True).reshape(size, width)
    half = size // 2
    after = shift(own, "y", -1)
    before = shift(own, "y", 1)
    far_a = shift(after[:half], "y", -1)
    far_b = shift(before[half:], "y", 1)
    far = jnp.concatenate([far_a, far_b], axis=0)
    blocks = [near(block) for block in (own, after, far, before)]

    scores = None
    anchors = [None] * ny
    for slot in (0, 1, 3, 2):
        index = local[:, slot * size : (slot + 1) * size]
        scores, anchors[slot] = score_block(gallery, blocks[slot], index, scores, slot, ny)
    stored = pltpu.with_memory_space_constraint(scores, pltpu.MemorySpace.HBM)
    scores = near(scores)
    anchors = summed_over_gallery(jnp.concatenate(anchors, axis=1))
    stats = summed_over_gallery(rank_sums(scores, anchors))

    weights = functools.partial(weight_blocks, cutoffs, stored, anchors, local, stats, gallery.T)
    dscore, part_far = weights(None, (2,), ny, BF16)
    dscore = near(dscore)
    got_a = shift(part_far[:half], "y", 1)
    got_b = shift(part_far[half:], "y", -1)
    dscore, part_next = weights(dscore, (1, 3), ny, F32)
    dscore = near(dscore)
    part_after, part_before = part_next[:size], part_next[size:]
    up = jnp.concatenate([part_after[:half] + got_a.astype(F32), part_after[half:]], axis=0).astype(BF16)
    down = jnp.concatenate([part_before[:half], part_before[half:] + got_b.astype(F32)], axis=0).astype(BF16)
    dscore, up, down = lax.optimization_barrier((dscore, up, down))
    got_up = shift(up, "y", 1)
    got_down = shift(down, "y", -1)
    dscore, part_own = weights(dscore, (0,), ny, F32)
    gallery_part = gallery_terms(near(dscore), blocks)

    out_rows = gallery_rows // (2 * nx)
    split = gallery_part.reshape(nx, 2, out_rows, width)
    core = lax.axis_index("c")
    mine = lax.dynamic_index_in_dim(split, core, 1, False)
    other = lax.dynamic_index_in_dim(split, 1 - core, 1, False).astype(BF16)
    pair = mine + lax.ppermute(other, "c", [(0, 1), (1, 0)]).astype(F32)
    xx = lax.axis_index("x")
    gallery_grad = lax.dynamic_index_in_dim(pair, xx, 0, False)
    sent = [
        shift(lax.dynamic_index_in_dim(pair, (xx + k) % nx, 0, False).astype(BF16), "x", k) for k in range(1, nx)
    ]
    for part in sent:
        gallery_grad = gallery_grad + part.astype(F32)

    query_part = (part_own + got_up.astype(F32) + got_down.astype(F32)).astype(BF16)
    landed = lax.all_to_all(query_part.reshape(nz, size // nz, width), "z", 0, 0, tiled=True)
    query_grad = jnp.sum(landed.astype(F32), axis=0)
    return (query_grad, gallery_grad)


def solution(mesh):
    fine = Mesh(mesh.devices.reshape(4, 2, 4, 8), ("x", "c", "y", "z"))
    placed = (P(("x", "c", "y", "z"), None), P(("y", "z"), None), P(("x", "c"), None), P())
    return jax.shard_map(
        shard_terms,
        mesh=fine,
        in_specs=placed,
        out_specs=(P(("x", "c", "y", "z"), None), P(("y", "z", "x", "c"), None)),
        check_vma=False,
    )
```

```python
import functools

import jax
import jax.numpy as jnp
from jax import lax
from jax.experimental import pallas as pl
from jax.experimental.pallas import tpu as pltpu
from jax.sharding import Mesh, PartitionSpec as P

TEMP = 0.05
SHARP = 4.0
HALF_INV = 0.5 / TEMP
TILE = 256
CHUNK = 64
F32 = jnp.float32
BF16 = jnp.bfloat16


def priced(micros):
    return pl.CostEstimate(flops=int(micros * 5e8), transcendentals=0, bytes_accessed=int(micros * 1e6))


def near(value):
    return pltpu.with_memory_space_constraint(value, pltpu.MemorySpace.VMEM)


def shift(value, axis, step):
    peers = lax.axis_size(axis)
    return lax.ppermute(value, axis, [(i, (i + step) % peers) for i in range(peers)])


def score_body(*refs):
    gallery_ref, query_ref, index_ref, score_ref, anchor_ref = refs[-5:]
    rows, lanes = score_ref.shape
    members = index_ref.shape[0]
    score_ref[...] = (
        lax.dot_general(gallery_ref[...], query_ref[...], (((1,), (1,)), ((), ())), preferred_element_type=F32)
        * HALF_INV
    )
    iota = lax.broadcasted_iota(jnp.int32, (CHUNK, lanes), 0)

    def step(i, found):
        base = i * CHUNK
        part = score_ref[pl.ds(pl.multiple_of(base, CHUNK), CHUNK), :]
        new = []
        for m in range(members):
            wanted = index_ref[m : m + 1, :] - base
            best = found[m]
            for row in range(0, CHUNK, 8):
                best = jnp.where(iota[row : row + 8] == wanted, part[row : row + 8], best)
            new.append(best)
        return tuple(new)

    zero = jnp.zeros((8, lanes), F32)
    found = lax.fori_loop(0, rows // CHUNK, step, (zero,) * members)
    for m in range(members):
        anchor_ref[m : m + 1, :] = jnp.sum(found[m], axis=0, keepdims=True)


def score_block(gallery, queries, index, carried, slot, slots):
    rows, width = gallery.shape
    count = queries.shape[0]
    members = index.shape[0]
    steps = count // TILE
    here = lambda i: (0, slot * steps + i)
    in_specs = [
        pl.BlockSpec((rows, width), lambda i: (0, 0)),
        pl.BlockSpec((TILE, width), lambda i: (i, 0)),
        pl.BlockSpec((members, TILE), lambda i: (0, i)),
    ]
    args = [gallery, queries, index]
    aliases = {}
    if carried is not None:
        in_specs = [pl.BlockSpec(memory_space=pl.ANY)] * 2 + in_specs
        args = [*carried, *args]
        aliases = {0: 0, 1: 1}
    return pl.pallas_call(
        score_body,
        grid=(steps,),
        in_specs=in_specs,
        out_specs=[
            pl.BlockSpec((rows, TILE), here),
            pl.BlockSpec((members, TILE), here),
        ],
        out_shape=[
            jax.ShapeDtypeStruct((rows, slots * count), F32),
            jax.ShapeDtypeStruct((members, slots * count), F32),
        ],
        input_output_aliases=aliases,
        cost_estimate=priced(5),
        compiler_params=pltpu.CompilerParams(vmem_limit_bytes=12 * 2**20),
    )(*args)


def rank_body(score_ref, anchor_ref, stat_ref):
    rows, lanes = score_ref.shape
    members = anchor_ref.shape[0]
    groups = CHUNK // 8
    for lane in range(0, lanes, 128):
        anchors = [anchor_ref[m : m + 1, lane : lane + 128] for m in range(members)]

        def step(i, sums):
            part = score_ref[pl.ds(pl.multiple_of(i * CHUNK, CHUNK), CHUNK), lane : lane + 128]
            new = []
            for m in range(members):
                t = jnp.tanh(part - anchors[m])
                new.append(sums[2 * m] + (jnp.sum(t.reshape(groups, 8, 128), axis=0) + float(groups)))
                new.append(sums[2 * m + 1] + (float(groups) - jnp.sum((t * t).reshape(groups, 8, 128), axis=0)))
            return tuple(new)

        zero = jnp.zeros((8, 128), F32)
        sums = lax.fori_loop(0, rows // CHUNK, step, (zero,) * (2 * members), unroll=4)
        for m in range(members):
            stat_ref[m : m + 1, lane : lane + 128] = 0.5 * jnp.sum(sums[2 * m], axis=0, keepdims=True)
            stat_ref[members + m : members + m + 1, lane : lane + 128] = 0.25 * jnp.sum(
                sums[2 * m + 1], axis=0, keepdims=True
            )


def rank_sums(scores, anchors):
    rows, count = scores.shape
    members = anchors.shape[0]
    return pl.pallas_call(
        rank_body,
        grid=(count // TILE,),
        in_specs=[
            pl.BlockSpec((rows, TILE), lambda i: (0, i)),
            pl.BlockSpec((members, TILE), lambda i: (0, i)),
        ],
        out_specs=pl.BlockSpec((2 * members, TILE), lambda i: (0, i)),
        out_shape=jax.ShapeDtypeStruct((2 * members, count), F32),
        cost_estimate=priced(12),
        compiler_params=pltpu.CompilerParams(vmem_limit_bytes=8 * 2**20),
        name="rank_sums",
    )(scores, anchors)


def weight_body(*refs):
    cut_ref, score_ref, anchor_ref, index_ref, stat_ref, gallery_ref, dscore_ref, query_ref, coef_ref = refs[-9:]
    rows, lanes = score_ref.shape
    members = anchor_ref.shape[0]
    cuts = cut_ref.shape[0]
    rank = 0.5 + stat_ref[0:members, :]
    slope = stat_ref[members : 2 * members, :] / TEMP
    weight = jnp.zeros((members, lanes), F32)
    for c in range(cuts):
        cut = cut_ref[c].astype(F32)
        decay = jnp.exp(-jnp.abs(SHARP * (cut - rank) / cut))
        weight = weight + decay / ((1.0 + decay) * (1.0 + decay)) * (SHARP / cut)
    weight = weight / float(members * cuts)
    scaled = weight * (0.25 / TEMP)
    coef_ref[0:members, :] = scaled
    coef_ref[members : 2 * members, :] = weight * slope
    total = jnp.sum(scaled, axis=0, keepdims=True)
    iota = lax.broadcasted_iota(jnp.int32, (CHUNK, 128), 0)
    for lane in range(0, lanes, 128):
        span = slice(lane, lane + 128)
        base_total = total[:, span]

        def step(i, carry):
            base = pl.multiple_of(i * CHUNK, CHUNK)
            part = score_ref[pl.ds(base, CHUNK), span]
            acc = jnp.broadcast_to(base_total, (CHUNK, 128))
            for m in range(members):
                t = jnp.tanh(part - anchor_ref[m : m + 1, span])
                hit = iota == (index_ref[m : m + 1, span] - base)
                acc = acc - jnp.where(
                    hit, coef_ref[members + m : members + m + 1, span], coef_ref[m : m + 1, span] * (t * t)
                )
            dscore_ref[pl.ds(base, CHUNK), span] = acc.astype(BF16)
            return carry

        lax.fori_loop(0, rows // CHUNK, step, 0, unroll=4)
    turned = jnp.dot(gallery_ref[...], dscore_ref[...], preferred_element_type=F32)
    query_ref[...] = turned.T.astype(query_ref.dtype)


def weight_blocks(cutoffs, scores, anchors, index, stats, turned, dscore, which, slots, dtype):
    width, rows = turned.shape
    members = anchors.shape[0]
    count = scores.shape[1] // slots
    steps = count // TILE
    stride = which[-1] - which[0] if len(which) > 1 else 0
    here = lambda i: (0, (which[0] + stride * (i // steps)) * steps + i % steps)
    in_specs = [
        pl.BlockSpec(memory_space=pltpu.SMEM),
        pl.BlockSpec((rows, TILE), here),
        pl.BlockSpec((members, TILE), here),
        pl.BlockSpec((members, TILE), here),
        pl.BlockSpec((2 * members, TILE), here),
        pl.BlockSpec((width, rows), lambda i: (0, 0)),
    ]
    args = [cutoffs, scores, anchors, index, stats, turned]
    aliases = {}
    if dscore is not None:
        in_specs = [pl.BlockSpec(memory_space=pl.ANY), *in_specs]
        args = [dscore, *args]
        aliases = {0: 0}
    return pl.pallas_call(
        weight_body,
        grid=(steps * len(which),),
        in_specs=in_specs,
        out_specs=[pl.BlockSpec((rows, TILE), here), pl.BlockSpec((TILE, width), lambda i: (i, 0))],
        out_shape=[
            jax.ShapeDtypeStruct((rows, slots * count), BF16),
            jax.ShapeDtypeStruct((len(which) * count, width), dtype),
        ],
        scratch_shapes=[pltpu.VMEM((2 * members, TILE), F32)],
        input_output_aliases=aliases,
        cost_estimate=priced(6 * len(which)),
        compiler_params=pltpu.CompilerParams(vmem_limit_bytes=16 * 2**20),
    )(*args)


def join_body(part_ref, low_ref, high_ref, up_ref, down_ref):
    half = low_ref.shape[0]
    size = 2 * half
    up_ref[0:half, :] = (part_ref[0:half, :] + low_ref[...].astype(F32)).astype(BF16)
    up_ref[half:size, :] = part_ref[half:size, :].astype(BF16)
    down_ref[0:half, :] = part_ref[size : size + half, :].astype(BF16)
    down_ref[half:size, :] = (part_ref[size + half : 2 * size, :] + high_ref[...].astype(F32)).astype(BF16)


def joined(part, low, high):
    out = jax.ShapeDtypeStruct((part.shape[0] // 2, part.shape[1]), BF16)
    return pl.pallas_call(
        join_body,
        out_shape=[out, out],
        compiler_params=pltpu.CompilerParams(vmem_limit_bytes=8 * 2**20),
        cost_estimate=priced(1),
        name="joined",
    )(part, low, high)


def gallery_body(dscore_ref, *refs):
    out_ref = refs[-1]
    at = 0
    acc = None
    for query_ref in refs[:-1]:
        size = query_ref.shape[0]
        term = jnp.dot(dscore_ref[:, at : at + size], query_ref[...], preferred_element_type=F32)
        acc = term if acc is None else acc + term
        at += size
    out_ref[...] = acc.astype(out_ref.dtype)


def gallery_terms(dscore, parts):
    rows, count = dscore.shape
    width = parts[0].shape[1]
    tile = rows // 3
    return pl.pallas_call(
        gallery_body,
        grid=(rows // tile,),
        in_specs=[
            pl.BlockSpec((tile, count), lambda i: (i, 0)),
            *[pl.BlockSpec(p.shape, lambda i: (0, 0)) for p in parts],
        ],
        out_specs=pl.BlockSpec((tile, width), lambda i: (i, 0)),
        out_shape=jax.ShapeDtypeStruct((rows, width), F32),
        cost_estimate=priced(6),
        compiler_params=pltpu.CompilerParams(vmem_limit_bytes=20 * 2**20),
        name="gallery_terms",
    )(dscore, *parts)


def summed_over_gallery(value):
    size = value.shape[1] // lax.axis_size("y")
    parts = [jnp.roll(shift(value, "y", k), -k * size, axis=1) for k in range(1, lax.axis_size("y"))]
    for part in parts:
        value = value + part
    lower = shift(value, "z", 1)
    upper = shift(value, "z", -1)
    two = value + lower
    three = two + upper
    return three + shift(three, "z", 3) + shift(two, "z", -3)


def shard_terms(queries, gallery, positives, cutoffs):
    ny = lax.axis_size("y")
    nz = lax.axis_size("z")
    nx = lax.axis_size("x")
    yy = lax.axis_index("y")
    gallery_rows, width = gallery.shape
    first_row = (yy * nz + lax.axis_index("z")) * gallery_rows
    local = positives.T - first_row
    size = local.shape[1] // ny
    local = lax.dynamic_slice_in_dim(jnp.concatenate([local, local], axis=1), yy * size, ny * size, 1)

    copies = jnp.broadcast_to(queries[None], (nz, *queries.shape))
    own = lax.all_to_all(copies, "z", 0, 0, tiled=True).reshape(size, width)
    half = size // 2
    after = shift(own, "y", -1)
    before = shift(own, "y", 1)
    far_a = shift(after[:half], "y", -1)
    far_b = shift(before[half:], "y", 1)
    far = jnp.concatenate([far_a, far_b], axis=0)
    blocks = [near(block) for block in (own, after, far, before)]

    carried = None
    for slot in (0, 1, 3, 2):
        index = local[:, slot * size : (slot + 1) * size]
        carried = score_block(gallery, blocks[slot], index, carried, slot, ny)
    scores, anchors = carried
    stored = pltpu.with_memory_space_constraint(scores, pltpu.MemorySpace.HBM)
    scores = near(scores)
    anchors = summed_over_gallery(anchors)
    stats = summed_over_gallery(rank_sums(scores, anchors))

    weights = functools.partial(weight_blocks, cutoffs, stored, anchors, local, stats, gallery.T)
    dscore, part_far = weights(None, (2,), ny, BF16)
    dscore = near(dscore)
    got_a = shift(part_far[:half], "y", 1)
    got_b = shift(part_far[half:], "y", -1)
    dscore, part_next = weights(dscore, (1, 3), ny, F32)
    dscore = near(dscore)
    up, down = joined(part_next, got_a, got_b)
    dscore, up, down = lax.optimization_barrier((dscore, up, down))
    got_up = shift(up, "y", 1)
    got_down = shift(down, "y", -1)
    dscore, part_own = weights(dscore, (0,), ny, F32)
    gallery_part = gallery_terms(near(dscore), blocks)

    out_rows = gallery_rows // (2 * nx)
    split = gallery_part.reshape(nx, 2, out_rows, width)
    core = lax.axis_index("c")
    mine = lax.dynamic_index_in_dim(split, core, 1, False)
    other = lax.dynamic_index_in_dim(split, 1 - core, 1, False).astype(BF16)
    pair = mine + lax.ppermute(other, "c", [(0, 1), (1, 0)]).astype(F32)
    xx = lax.axis_index("x")
    gallery_grad = lax.dynamic_index_in_dim(pair, xx, 0, False)
    sent = [
        shift(lax.dynamic_index_in_dim(pair, (xx + k) % nx, 0, False).astype(BF16), "x", k) for k in range(1, nx)
    ]
    for part in sent:
        gallery_grad = gallery_grad + part.astype(F32)

    query_part = (part_own + got_up.astype(F32) + got_down.astype(F32)).astype(BF16)
    landed = lax.all_to_all(query_part.reshape(nz, size // nz, width), "z", 0, 0, tiled=True)
    query_grad = jnp.sum(landed.astype(F32), axis=0)
    return (query_grad, gallery_grad)


def solution(mesh):
    fine = Mesh(mesh.devices.reshape(4, 2, 4, 8), ("x", "c", "y", "z"))
    placed = (P(("x", "c", "y", "z"), None), P(("y", "z"), None), P(("x", "c"), None), P())
    return jax.shard_map(
        shard_terms,
        mesh=fine,
        in_specs=placed,
        out_specs=(P(("x", "c", "y", "z"), None), P(("y", "z", "x", "c"), None)),
        check_vma=False,
    )
```

```python
import functools

import jax
import jax.numpy as jnp
from jax import lax
from jax.experimental import pallas as pl
from jax.experimental.pallas import tpu as pltpu
from jax.sharding import Mesh, PartitionSpec as P

TEMP = 0.05
SHARP = 4.0
HALF_INV = 0.5 / TEMP
TILE = 256
CHUNK = 64
F32 = jnp.float32
BF16 = jnp.bfloat16


def priced(micros):
    return pl.CostEstimate(flops=int(micros * 5e8), transcendentals=0, bytes_accessed=int(micros * 1e6))


def near(value):
    return pltpu.with_memory_space_constraint(value, pltpu.MemorySpace.VMEM)


def shift(value, axis, step):
    peers = lax.axis_size(axis)
    return lax.ppermute(value, axis, [(i, (i + step) % peers) for i in range(peers)])


def score_body(*refs):
    gallery_ref, query_ref, index_ref, score_ref, anchor_ref = refs[-5:]
    rows, lanes = score_ref.shape
    members = index_ref.shape[0]
    score_ref[...] = (
        lax.dot_general(gallery_ref[...], query_ref[...], (((1,), (1,)), ((), ())), preferred_element_type=F32)
        * HALF_INV
    )
    iota = lax.broadcasted_iota(jnp.int32, (CHUNK, lanes), 0)

    def step(i, found):
        base = i * CHUNK
        part = score_ref[pl.ds(pl.multiple_of(base, CHUNK), CHUNK), :]
        new = []
        for m in range(members):
            wanted = index_ref[m : m + 1, :] - base
            best = found[m]
            for row in range(0, CHUNK, 8):
                best = jnp.where(iota[row : row + 8] == wanted, part[row : row + 8], best)
            new.append(best)
        return tuple(new)

    zero = jnp.zeros((8, lanes), F32)
    found = lax.fori_loop(0, rows // CHUNK, step, (zero,) * members)
    for m in range(members):
        anchor_ref[m : m + 1, :] = jnp.sum(found[m], axis=0, keepdims=True)


def score_block(gallery, queries, index, carried, slot, slots):
    rows, width = gallery.shape
    count = queries.shape[0]
    members = index.shape[0]
    steps = count // TILE
    here = lambda i: (0, slot * steps + i)
    in_specs = [
        pl.BlockSpec((rows, width), lambda i: (0, 0)),
        pl.BlockSpec((TILE, width), lambda i: (i, 0)),
        pl.BlockSpec((members, TILE), lambda i: (0, i)),
    ]
    args = [gallery, queries, index]
    aliases = {}
    if carried is not None:
        in_specs = [pl.BlockSpec(memory_space=pl.ANY)] * 2 + in_specs
        args = [*carried, *args]
        aliases = {0: 0, 1: 1}
    return pl.pallas_call(
        score_body,
        grid=(steps,),
        in_specs=in_specs,
        out_specs=[
            pl.BlockSpec((rows, TILE), here),
            pl.BlockSpec((members, TILE), here),
        ],
        out_shape=[
            jax.ShapeDtypeStruct((rows, slots * count), F32),
            jax.ShapeDtypeStruct((members, slots * count), F32),
        ],
        input_output_aliases=aliases,
        cost_estimate=priced(5),
        compiler_params=pltpu.CompilerParams(vmem_limit_bytes=12 * 2**20),
    )(*args)


def rank_body(score_ref, three_ref, low_ref, high_ref, stat_ref, anchor_ref):
    rows, lanes = score_ref.shape
    anchor_ref[...] = three_ref[...] + low_ref[...] + high_ref[...]
    members = anchor_ref.shape[0]
    groups = CHUNK // 8
    for lane in range(0, lanes, 128):
        anchors = [anchor_ref[m : m + 1, lane : lane + 128] for m in range(members)]

        def step(i, sums):
            part = score_ref[pl.ds(pl.multiple_of(i * CHUNK, CHUNK), CHUNK), lane : lane + 128]
            new = []
            for m in range(members):
                t = jnp.tanh(part - anchors[m])
                new.append(sums[2 * m] + (jnp.sum(t.reshape(groups, 8, 128), axis=0) + float(groups)))
                new.append(sums[2 * m + 1] + (float(groups) - jnp.sum((t * t).reshape(groups, 8, 128), axis=0)))
            return tuple(new)

        zero = jnp.zeros((8, 128), F32)
        sums = lax.fori_loop(0, rows // CHUNK, step, (zero,) * (2 * members), unroll=4)
        for m in range(members):
            stat_ref[m : m + 1, lane : lane + 128] = 0.5 * jnp.sum(sums[2 * m], axis=0, keepdims=True)
            stat_ref[members + m : members + m + 1, lane : lane + 128] = 0.25 * jnp.sum(
                sums[2 * m + 1], axis=0, keepdims=True
            )


def rank_sums(scores, anchors):
    rows, count = scores.shape
    members = anchors[0].shape[0]
    row_spec = pl.BlockSpec((members, TILE), lambda i: (0, i))
    return pl.pallas_call(
        rank_body,
        grid=(count // TILE,),
        in_specs=[
            pl.BlockSpec((rows, TILE), lambda i: (0, i)),
            row_spec,
            row_spec,
            row_spec,
        ],
        out_specs=[pl.BlockSpec((2 * members, TILE), lambda i: (0, i)), row_spec],
        out_shape=[
            jax.ShapeDtypeStruct((2 * members, count), F32),
            jax.ShapeDtypeStruct((members, count), F32),
        ],
        cost_estimate=priced(12),
        compiler_params=pltpu.CompilerParams(vmem_limit_bytes=8 * 2**20),
        name="rank_sums",
    )(scores, *anchors)


def weight_body(*refs):
    cut_ref, score_ref, anchor_ref, index_ref, three_ref, low_ref, high_ref, gallery_ref = refs[-11:-3]
    dscore_ref, query_ref, coef_ref = refs[-3:]
    stats = three_ref[...] + low_ref[...] + high_ref[...]
    rows, lanes = score_ref.shape
    members = anchor_ref.shape[0]
    cuts = cut_ref.shape[0]
    rank = 0.5 + stats[0:members]
    slope = stats[members : 2 * members] / TEMP
    weight = jnp.zeros((members, lanes), F32)
    for c in range(cuts):
        cut = cut_ref[c].astype(F32)
        decay = jnp.exp(-jnp.abs(SHARP * (cut - rank) / cut))
        weight = weight + decay / ((1.0 + decay) * (1.0 + decay)) * (SHARP / cut)
    weight = weight / float(members * cuts)
    scaled = weight * (0.25 / TEMP)
    coef_ref[0:members, :] = scaled
    coef_ref[members : 2 * members, :] = weight * slope
    total = jnp.sum(scaled, axis=0, keepdims=True)
    iota = lax.broadcasted_iota(jnp.int32, (CHUNK, 128), 0)
    for lane in range(0, lanes, 128):
        span = slice(lane, lane + 128)
        base_total = total[:, span]

        def step(i, carry):
            base = pl.multiple_of(i * CHUNK, CHUNK)
            part = score_ref[pl.ds(base, CHUNK), span]
            acc = jnp.broadcast_to(base_total, (CHUNK, 128))
            for m in range(members):
                t = jnp.tanh(part - anchor_ref[m : m + 1, span])
                hit = iota == (index_ref[m : m + 1, span] - base)
                acc = acc - jnp.where(
                    hit, coef_ref[members + m : members + m + 1, span], coef_ref[m : m + 1, span] * (t * t)
                )
            dscore_ref[pl.ds(base, CHUNK), span] = acc.astype(BF16)
            return carry

        lax.fori_loop(0, rows // CHUNK, step, 0, unroll=4)
    turned = jnp.dot(gallery_ref[...], dscore_ref[...], preferred_element_type=F32)
    query_ref[...] = turned.T.astype(query_ref.dtype)


def weight_blocks(cutoffs, scores, anchors, index, stats, turned, dscore, which, slots, dtype):
    width, rows = turned.shape
    members = anchors.shape[0]
    count = scores.shape[1] // slots
    steps = count // TILE
    stride = which[-1] - which[0] if len(which) > 1 else 0
    here = lambda i: (0, (which[0] + stride * (i // steps)) * steps + i % steps)
    in_specs = [
        pl.BlockSpec(memory_space=pltpu.SMEM),
        pl.BlockSpec((rows, TILE), here),
        pl.BlockSpec((members, TILE), here),
        pl.BlockSpec((members, TILE), here),
        *[pl.BlockSpec((2 * members, TILE), here)] * 3,
        pl.BlockSpec((width, rows), lambda i: (0, 0)),
    ]
    args = [cutoffs, scores, anchors, index, *stats, turned]
    aliases = {}
    if dscore is not None:
        in_specs = [pl.BlockSpec(memory_space=pl.ANY), *in_specs]
        args = [dscore, *args]
        aliases = {0: 0}
    return pl.pallas_call(
        weight_body,
        grid=(steps * len(which),),
        in_specs=in_specs,
        out_specs=[pl.BlockSpec((rows, TILE), here), pl.BlockSpec((TILE, width), lambda i: (i, 0))],
        out_shape=[
            jax.ShapeDtypeStruct((rows, slots * count), BF16),
            jax.ShapeDtypeStruct((len(which) * count, width), dtype),
        ],
        scratch_shapes=[pltpu.VMEM((2 * members, TILE), F32)],
        input_output_aliases=aliases,
        cost_estimate=priced(6 * len(which)),
        compiler_params=pltpu.CompilerParams(vmem_limit_bytes=16 * 2**20),
    )(*args)


def join_body(part_ref, low_ref, high_ref, up_ref, down_ref):
    half = low_ref.shape[0]
    size = 2 * half
    up_ref[0:half, :] = (part_ref[0:half, :] + low_ref[...].astype(F32)).astype(BF16)
    up_ref[half:size, :] = part_ref[half:size, :].astype(BF16)
    down_ref[0:half, :] = part_ref[size : size + half, :].astype(BF16)
    down_ref[half:size, :] = (part_ref[size + half : 2 * size, :] + high_ref[...].astype(F32)).astype(BF16)


def joined(part, low, high):
    out = jax.ShapeDtypeStruct((part.shape[0] // 2, part.shape[1]), BF16)
    return pl.pallas_call(
        join_body,
        out_shape=[out, out],
        compiler_params=pltpu.CompilerParams(vmem_limit_bytes=8 * 2**20),
        cost_estimate=priced(1),
        name="joined",
    )(part, low, high)


def gallery_body(dscore_ref, *refs):
    out_ref = refs[-1]
    at = 0
    acc = None
    for query_ref in refs[:-1]:
        size = query_ref.shape[0]
        term = jnp.dot(dscore_ref[:, at : at + size], query_ref[...], preferred_element_type=F32)
        acc = term if acc is None else acc + term
        at += size
    out_ref[...] = acc.astype(out_ref.dtype)


def gallery_terms(dscore, parts):
    rows, count = dscore.shape
    width = parts[0].shape[1]
    tile = rows // 3
    return pl.pallas_call(
        gallery_body,
        grid=(rows // tile,),
        in_specs=[
            pl.BlockSpec((tile, count), lambda i: (i, 0)),
            *[pl.BlockSpec(p.shape, lambda i: (0, 0)) for p in parts],
        ],
        out_specs=pl.BlockSpec((tile, width), lambda i: (i, 0)),
        out_shape=jax.ShapeDtypeStruct((rows, width), F32),
        cost_estimate=priced(6),
        compiler_params=pltpu.CompilerParams(vmem_limit_bytes=20 * 2**20),
        name="gallery_terms",
    )(dscore, *parts)


def summed_over_gallery(value):
    size = value.shape[1] // lax.axis_size("y")
    parts = [jnp.roll(shift(value, "y", k), -k * size, axis=1) for k in range(1, lax.axis_size("y"))]
    for part in parts:
        value = value + part
    lower = shift(value, "z", 1)
    upper = shift(value, "z", -1)
    two = value + lower
    three = two + upper
    return three, shift(three, "z", 3), shift(two, "z", -3)


def shard_terms(queries, gallery, positives, cutoffs):
    ny = lax.axis_size("y")
    nz = lax.axis_size("z")
    nx = lax.axis_size("x")
    yy = lax.axis_index("y")
    gallery_rows, width = gallery.shape
    first_row = (yy * nz + lax.axis_index("z")) * gallery_rows
    local = positives.T - first_row
    size = local.shape[1] // ny
    local = lax.dynamic_slice_in_dim(jnp.concatenate([local, local], axis=1), yy * size, ny * size, 1)

    copies = jnp.broadcast_to(queries[None], (nz, *queries.shape))
    own = lax.all_to_all(copies, "z", 0, 0, tiled=True).reshape(size, width)
    half = size // 2
    after = shift(own, "y", -1)
    before = shift(own, "y", 1)
    far_a = shift(after[:half], "y", -1)
    far_b = shift(before[half:], "y", 1)
    far = jnp.concatenate([far_a, far_b], axis=0)
    blocks = [near(block) for block in (own, after, far, before)]

    carried = None
    for slot in (0, 1, 3, 2):
        index = local[:, slot * size : (slot + 1) * size]
        carried = score_block(gallery, blocks[slot], index, carried, slot, ny)
    scores, anchors = carried
    stored = pltpu.with_memory_space_constraint(scores, pltpu.MemorySpace.HBM)
    scores = near(scores)
    stats, anchors = rank_sums(scores, summed_over_gallery(anchors))
    stats = summed_over_gallery(stats)

    weights = functools.partial(weight_blocks, cutoffs, stored, anchors, local, stats, gallery.T)
    dscore, part_far = weights(None, (2,), ny, BF16)
    dscore = near(dscore)
    got_a = shift(part_far[:half], "y", 1)
    got_b = shift(part_far[half:], "y", -1)
    dscore, part_next = weights(dscore, (1, 3), ny, F32)
    dscore = near(dscore)
    up, down = joined(part_next, got_a, got_b)
    dscore, up, down = lax.optimization_barrier((dscore, up, down))
    got_up = shift(up, "y", 1)
    got_down = shift(down, "y", -1)
    dscore, part_own = weights(dscore, (0,), ny, F32)
    gallery_part = gallery_terms(near(dscore), blocks)

    out_rows = gallery_rows // (2 * nx)
    split = gallery_part.reshape(nx, 2, out_rows, width)
    core = lax.axis_index("c")
    mine = lax.dynamic_index_in_dim(split, core, 1, False)
    other = lax.dynamic_index_in_dim(split, 1 - core, 1, False).astype(BF16)
    pair = mine + lax.ppermute(other, "c", [(0, 1), (1, 0)]).astype(F32)
    xx = lax.axis_index("x")
    gallery_grad = lax.dynamic_index_in_dim(pair, xx, 0, False)
    sent = [
        shift(lax.dynamic_index_in_dim(pair, (xx + k) % nx, 0, False).astype(BF16), "x", k) for k in range(1, nx)
    ]
    for part in sent:
        gallery_grad = gallery_grad + part.astype(F32)

    query_part = (part_own + got_up.astype(F32) + got_down.astype(F32)).astype(BF16)
    landed = lax.all_to_all(query_part.reshape(nz, size // nz, width), "z", 0, 0, tiled=True)
    query_grad = jnp.sum(landed.astype(F32), axis=0)
    return (query_grad, gallery_grad)


def solution(mesh):
    fine = Mesh(mesh.devices.reshape(4, 2, 4, 8), ("x", "c", "y", "z"))
    placed = (P(("x", "c", "y", "z"), None), P(("y", "z"), None), P(("x", "c"), None), P())
    return jax.shard_map(
        shard_terms,
        mesh=fine,
        in_specs=placed,
        out_specs=(P(("x", "c", "y", "z"), None), P(("y", "z", "x", "c"), None)),
        check_vma=False,
    )
```
